32 devices in a mesh: ccy: 4 (over x, core), path: 8 (over z, y).
Axes of the slice: x: 2, y: 2, z: 4, core: 2. Of those that a mesh axis runs over, the one named last changes fastest.
Arguments:
- curve_store: bfloat16 [4, 16, 64, 2048], P('ccy', 'path'), may hold values from -0.13 to 0.18
- cash_index: int32 [4, 2048, 16], P('ccy'), may hold values from 0 to 1023
- cash_amount: float32 [4, 2048, 16], P('ccy'), may hold values from -0.6 to 0.6
- trade_set: int32 [4, 2048], P('ccy'), may hold values from 0 to 511
- date_slot: int32 [16], replicated, may hold values from 0 to 15, as said below
- default_weight: float32 [16, 512], replicated, may hold values from 0.02 to 0.2
Outputs:
- exposure: float32 [16, 512], P(None, 'ccy')
- node_sens: float32 [4, 16, 64], P('ccy')
The draws below stay inside these ranges and needn't reach their ends.
Inputs may be any that keep to these rules, and one draw needn't show every extreme that they name: `date_slot`: the 16 slots are distinct; slot s is stored at path index s // 2, position s % 2.
All inputs are finite; a program needn't handle non-finite values.
Results may differ from the reference program's by a relative error of at most 0.0029.
Values may be sent and summed in bfloat16 or wider, within the bound.
A program may use at most 64 MiB of HBM per device.

```python
import math
import jax
import jax.numpy as jnp
from jax import lax

NODES = 64
CFG = 1024
NSETS = 512
TRADES = 2048
NCF = 16
DATES = 16
PATHS = 2048
SLOTS_ALL = 16
N_CCY = 4


def draw_date_slot(key, part):
    return jax.random.permutation(key, SLOTS_ALL)[:DATES].astype(jnp.int32)


def draw_curve_store(key, part):
    level_key, spread_key, height_key, flip_key = jax.random.split(jax.random.fold_in(key, 7), 4)
    block_shape = (N_CCY, SLOTS_ALL, 1, PATHS)
    base_level = jax.random.uniform(level_key, block_shape, jnp.float32, 0.0, 0.05)
    jump_scale = jnp.exp(jax.random.uniform(spread_key, block_shape, jnp.float32, math.log(0.01), math.log(0.12)))
    jump_height = jax.random.uniform(height_key, (N_CCY, SLOTS_ALL, NODES, PATHS), jnp.float32, 0.5, 1.0)
    flip_bits = jax.random.randint(flip_key, block_shape, 0, 2)
    node_index = jnp.arange(NODES, dtype=jnp.int32).reshape(1, 1, NODES, 1)
    parity = (node_index + flip_bits) % 2
    signed = 1.0 - 2.0 * parity.astype(jnp.float32)
    return (base_level + jump_scale * signed * jump_height).astype(jnp.bfloat16)


def touch_ends(drawn, key, least, largest):
    spot = [jax.random.randint(jax.random.fold_in(key, axis), (), 0, length) for axis, length in enumerate(drawn.shape)]
    main_axis = drawn.shape.index(max(drawn.shape))
    neighbour = spot[:main_axis] + [(spot[main_axis] + 1) % drawn.shape[main_axis]] + spot[main_axis + 1:]
    return drawn.at[tuple(spot)].set(least).at[tuple(neighbour)].set(largest)


def level_of(own_key, dims, shards, least, top_value):
    def one(dim, blocks):
        draws = jax.random.uniform(jax.random.fold_in(jax.random.fold_in(own_key, 6), dim), (blocks,), jnp.float32, least / len(shards), top_value / len(shards))
        return jnp.repeat(jnp.exp(draws), dims[dim] // blocks).reshape((-1,) + (1,) * (len(dims) - dim - 1))

    gain = one(*shards[0])
    for cut in shards[1:]:
        gain = gain * one(*cut)
    return gain


def noise(stream_key, extent, scale, most, shards=(), held_as=jnp.bfloat16):
    entries = jax.random.normal(stream_key, extent, jnp.float32) * scale
    if len(shards) > 0:
        entries = level_of(stream_key, extent, shards, -0.22, 0.18) * entries
    return jnp.clip(entries, min=-most, max=most).astype(held_as)


def setup_inputs(seed: int = 0) -> dict:
    key_list = jax.random.split(jax.random.key(seed), 7)
    return {
        "curve_store": draw_curve_store(jax.random.fold_in(key_list[6], 71), 0),
        "cash_index": touch_ends(jax.random.randint(key_list[1], (N_CCY, TRADES, NCF), 0, CFG), jax.random.fold_in(key_list[1], 1), 0, CFG - 1).astype(jnp.int32),
        "cash_amount": noise(key_list[2], (N_CCY, TRADES, NCF), 0.1, 0.6, ((0, 4),), jnp.float32),
        "trade_set": touch_ends(jax.random.randint(key_list[3], (N_CCY, TRADES), 0, NSETS), jax.random.fold_in(key_list[3], 1), 0, NSETS - 1).astype(jnp.int32),
        "date_slot": draw_date_slot(jax.random.fold_in(key_list[6], 71), 0),
        "default_weight": jnp.clip(jnp.exp(jax.random.uniform(key_list[5], (DATES, NSETS), jnp.float32, math.log(0.02), math.log(0.2))), 0.02, 0.2),
    }


SOFTEN = 0.04
HORIZON = 32.0

def date_tables(date_index, node_count, grid_count):
    start_time = 0.5 * (jnp.asarray(date_index).astype(jnp.float32) + 1.0)
    grid_times = HORIZON * (jnp.arange(grid_count, dtype=jnp.float32) + 1.0) / grid_count
    tenors = HORIZON * (jnp.arange(node_count, dtype=jnp.float32) + 1.0) / node_count
    remain = grid_times - start_time
    alive_mask = (remain > 0.0).astype(jnp.float32)
    clipped = jnp.clip(remain, HORIZON / node_count, HORIZON)
    weights = jnp.maximum(0.0, 1.0 - jnp.abs(clipped[None, :] - tenors[:, None]) * (node_count / HORIZON))
    return (remain, alive_mask, weights)

def netted_cash(flow_index, amount, trade_sets):
    columns = jnp.repeat(trade_sets, flow_index.shape[1]).astype(jnp.int32)
    cash_table = jnp.zeros((CFG, NSETS), jnp.float32).at[flow_index.reshape(-1).astype(jnp.int32), columns].add(amount.reshape(-1).astype(jnp.float32))
    return cash_table.astype(jnp.bfloat16)

def reference(curve_store, cash_index, cash_amount, trade_set, date_slot, default_weight):
    total_paths = curve_store.shape[3]
    tables = [netted_cash(cash_index[member], cash_amount[member], trade_set[member]) for member in range(N_CCY)]
    exposure_rows = []
    sens_rows = []
    for date_index in range(DATES):
        remain, alive_mask, weights = date_tables(date_index, NODES, CFG)
        grid_weights = weights.astype(jnp.bfloat16)
        values = jnp.zeros((total_paths, NSETS), jnp.float32)
        discounts = []
        for member in range(N_CCY):
            curve_now = lax.dynamic_index_in_dim(curve_store[member], date_slot[date_index].astype(jnp.int32), 0, keepdims=False)
            yields = lax.dot_general(curve_now, grid_weights, (((0,), (0,)), ((), ())), preferred_element_type=jnp.float32)
            discount = alive_mask * jnp.exp(-yields * remain)
            discounts.append(discount)
            values = values + jnp.dot(discount.astype(jnp.bfloat16), tables[member], preferred_element_type=jnp.float32)
        rooted = jnp.sqrt(values * values + SOFTEN)
        exposure_rows.append(lax.optimization_barrier(jnp.sum(0.5 * (values + rooted), axis=0)) / total_paths)
        slopes = (default_weight[date_index] / total_paths * 0.5 * (1.0 + values / rooted)).astype(jnp.bfloat16)
        group_sens = []
        for member in range(N_CCY):
            back_flow = lax.dot_general(slopes, tables[member], (((1,), (1,)), ((), ())), preferred_element_type=jnp.float32)
            node_pull = lax.optimization_barrier(jnp.sum(back_flow * -remain * discounts[member], axis=0))
            group_sens.append(jnp.dot(weights, node_pull, precision=lax.Precision.HIGHEST))
        sens_rows.append(jnp.stack(group_sens))
    return (jnp.stack(exposure_rows), jnp.stack(sens_rows, axis=1))
```

```python
import functools

import jax
import jax.numpy as jnp
from jax import lax
from jax.experimental import pallas as pl
from jax.experimental.pallas import tpu as pltpu
from jax.sharding import PartitionSpec as P

NSETS = 512
CFG = 1024
SOFTEN = 0.04
HORIZON = 32.0
LOG2E = 1.4426950408889634
COLS = 256


def date_tables(date_index, node_count, grid_count):
    start_time = 0.5 * (jnp.asarray(date_index).astype(jnp.float32) + 1.0)
    grid_times = HORIZON * (jnp.arange(grid_count, dtype=jnp.float32) + 1.0) / grid_count
    tenors = HORIZON * (jnp.arange(node_count, dtype=jnp.float32) + 1.0) / node_count
    remain = grid_times - start_time
    alive_mask = (remain > 0.0).astype(jnp.float32)
    clipped = jnp.clip(remain, HORIZON / node_count, HORIZON)
    weights = jnp.maximum(
        0.0, 1.0 - jnp.abs(clipped[None, :] - tenors[:, None]) * (node_count / HORIZON)
    )
    return (remain, alive_mask, weights)


def cash_kernel(rows, base_ref, index_ref, amount_ref, set_ref, out_ref, a_hi, a_lo):
    flows, trades = index_ref.shape
    nsets = out_ref.shape[1]
    wanted = lax.broadcasted_iota(jnp.int32, (rows, 128), 0) + base_ref[0]

    @pl.loop(0, trades // 128)
    def _(tile):
        cols = pl.ds(pl.multiple_of(tile * 128, 128), 128)
        total = jnp.zeros((rows, 128), jnp.float32)
        index = index_ref[:, cols]
        amount = amount_ref[:, cols]
        for k in range(flows):
            hit = wanted == index[k : k + 1, :]
            total = total + jnp.where(hit, amount[k : k + 1, :], 0.0)
        high = total.astype(jnp.bfloat16)
        a_hi[:, cols] = high
        a_lo[:, cols] = (total - high.astype(jnp.float32)).astype(jnp.bfloat16)

    sets = lax.broadcasted_iota(jnp.int32, (nsets, trades), 0)
    onehot = jnp.where(sets == set_ref[...], 1.0, 0.0).astype(jnp.bfloat16)
    dims = (((1,), (1,)), ((), ()))
    table = lax.dot_general(a_hi[...], onehot, dims, preferred_element_type=jnp.float32)
    table = table + lax.dot_general(a_lo[...], onehot, dims, preferred_element_type=jnp.float32)
    out_ref[...] = table.astype(jnp.bfloat16)


def build_cash(base, flow_index, amount, trade_sets, rows, nsets):
    flows, trades = flow_index.shape[1], flow_index.shape[0]
    vmem = pl.BlockSpec(memory_space=pltpu.VMEM)
    return pl.pallas_call(
        functools.partial(cash_kernel, rows),
        out_shape=jax.ShapeDtypeStruct((rows, nsets), jnp.bfloat16),
        in_specs=[pl.BlockSpec(memory_space=pltpu.SMEM), vmem, vmem, vmem],
        out_specs=vmem,
        scratch_shapes=[pltpu.VMEM((rows, trades), jnp.bfloat16)] * 2,
        cost_estimate=pl.CostEstimate(
            flops=4 * rows * trades * nsets, bytes_accessed=4 * trades * flows, transcendentals=0
        ),
        name="cash_rows",
    )(base, flow_index.T, amount.T, trade_sets[None, :])


def main_kernel(groups, cfg, total_paths, date_ref, curve_ref, cash_ref, dw_ref, exp_ref, sens_ref, disc):
    nodes, paths = curve_ref.shape[2], curve_ref.shape[3]
    date = date_ref[pl.program_id(0)]
    start_time = 0.5 * (date.astype(jnp.float32) + 1.0)
    step = HORIZON / cfg
    tenors = (lax.broadcasted_iota(jnp.int32, (nodes, COLS), 0).astype(jnp.float32) + 1.0) * (HORIZON / nodes)
    per_group = cfg // COLS

    def tables(block):
        at = lax.broadcasted_iota(jnp.int32, (1, COLS), 1) + block * COLS
        remain = (at.astype(jnp.float32) + 1.0) * step - start_time
        clipped = jnp.clip(remain, HORIZON / nodes, HORIZON)
        weights = jnp.maximum(0.0, 1.0 - jnp.abs(clipped - tenors) * (nodes / HORIZON))
        return remain, weights

    for block in range(per_group):
        remain, weights = tables(block)
        weights = weights.astype(jnp.bfloat16)
        scaled = remain * (-LOG2E)
        alive = remain > 0.0
        for g in range(groups):
            rate = lax.dot_general(
                curve_ref[g, 0], weights, (((0,), (0,)), ((), ())), preferred_element_type=jnp.float32
            )
            value = jnp.where(alive, jnp.exp2(rate * scaled), 0.0)
            disc[:, pl.ds(g * cfg + block * COLS, COLS)] = value.astype(jnp.bfloat16)

    values = jnp.dot(disc[...], cash_ref[...], preferred_element_type=jnp.float32)
    square = values * values + SOFTEN
    inverse = lax.rsqrt(square)
    exp_ref[0] = jnp.sum(0.5 * (values + square * inverse), axis=0, keepdims=True) / total_paths
    row = dw_ref[pl.ds(date, 1), :] / total_paths * 0.5
    slopes = (row * (1.0 + values * inverse)).astype(jnp.bfloat16)

    for g in range(groups):
        sens = jnp.zeros((8, nodes), jnp.float32)
        for block in range(per_group):
            at = g * cfg + block * COLS
            back = lax.dot_general(
                slopes, cash_ref[pl.ds(at, COLS), :], (((1,), (1,)), ((), ())),
                preferred_element_type=jnp.float32,
            )
            summed = jnp.sum(back * disc[:, pl.ds(at, COLS)].astype(jnp.float32), axis=0, keepdims=True)
            remain, weights = tables(block)
            pull = jnp.broadcast_to(summed * -remain, (8, COLS))
            weights = weights.astype(jnp.bfloat16)
            for _ in range(3):
                piece = pull.astype(jnp.bfloat16)
                pull = pull - piece.astype(jnp.float32)
                sens = sens + lax.dot_general(
                    piece, weights, (((1,), (1,)), ((), ())), preferred_element_type=jnp.float32
                )
        sens_ref[0, g : g + 1, :] = sens[0:1, :]


def run_main(dates, curves, cash, default_weight, total_paths):
    groups, slots, nodes, paths = curves.shape
    rows, nsets = cash.shape
    cfg = rows // groups
    work = slots * paths * rows * (4 * nsets + 2 * nodes)
    return pl.pallas_call(
        functools.partial(main_kernel, groups, cfg, total_paths),
        grid=(slots,),
        out_shape=[
            jax.ShapeDtypeStruct((slots, 1, nsets), jnp.float32),
            jax.ShapeDtypeStruct((slots, groups, nodes), jnp.float32),
        ],
        in_specs=[
            pl.BlockSpec(memory_space=pltpu.SMEM),
            pl.BlockSpec((groups, 1, nodes, paths), lambda s: (0, s, 0, 0)),
            pl.BlockSpec(memory_space=pltpu.VMEM),
            pl.BlockSpec(memory_space=pltpu.VMEM),
        ],
        out_specs=[
            pl.BlockSpec((1, 1, nsets), lambda s: (s, 0, 0)),
            pl.BlockSpec((1, groups, nodes), lambda s: (s, 0, 0)),
        ],
        scratch_shapes=[pltpu.VMEM((paths, rows), jnp.bfloat16)],
        cost_estimate=pl.CostEstimate(
            flops=work, bytes_accessed=rows * nsets * 2, transcendentals=slots * paths * rows
        ),
        name="price_dates",
    )(dates, curves, cash, default_weight)


def by_slot(curve_store, cash_index, cash_amount, trade_set, date_slot, default_weight):
    groups, members = lax.axis_size("ccy"), lax.axis_size("path")
    group_index, path_index = lax.axis_index("ccy"), lax.axis_index("path")
    slots = curve_store.shape[1]
    nodes = curve_store.shape[2]
    total_paths = curve_store.shape[3]
    rows = CFG // members
    nsets = default_weight.shape[1]
    base = (path_index * rows).astype(jnp.int32)[None]
    curves = lax.all_to_all(curve_store, "ccy", split_axis=3, concat_axis=0, tiled=True)
    chunk = build_cash(base, cash_index[0], cash_amount[0], trade_set[0], rows, nsets)
    cash = lax.all_gather(chunk, ("ccy", "path"), axis=0, tiled=True)
    own = path_index * slots + jnp.arange(slots, dtype=jnp.int32)
    numbers = jnp.arange(date_slot.shape[0], dtype=jnp.int32)
    dates = jnp.sum(jnp.where(date_slot[None, :] == own[:, None], numbers[None, :], 0), axis=1).astype(jnp.int32)
    exposure_part, sens_part = run_main(dates, curves, cash, default_weight, total_paths)
    part = jnp.concatenate([exposure_part[:, 0, :], sens_part.reshape(slots, groups * nodes)], axis=1)
    parts = lax.all_gather(part, ("ccy", "path"), axis=0)
    share = nsets // groups
    exposure = lax.dynamic_slice_in_dim(parts, group_index * share, share, 2)
    sens = lax.dynamic_slice_in_dim(parts, nsets + group_index * nodes, nodes, 2)

    def finish(block):
        rows_by_slot = jnp.sum(block.reshape(groups, members * slots, -1), axis=0)
        hit = date_slot[:, None, None] == jnp.arange(members * slots, dtype=jnp.int32)[None, :, None]
        return jnp.sum(jnp.where(hit, rows_by_slot[None], 0.0), axis=1)

    return (finish(exposure), finish(sens)[None])


def by_path(curve_store, cash_index, cash_amount, trade_set, date_slot, default_weight):
    groups = lax.axis_size("ccy")
    group_index = lax.axis_index("ccy")
    members = lax.axis_size("path")
    nodes, total_paths = curve_store.shape[2], curve_store.shape[3]
    nsets = default_weight.shape[1]
    share_size = nsets // groups
    rows = CFG // members
    base = (lax.axis_index("path") * rows).astype(jnp.int32)[None]
    chunk = build_cash(base, cash_index[0], cash_amount[0], trade_set[0], rows, nsets)
    cash_table = lax.all_gather(chunk, "path", axis=0, tiled=True)
    blocks = lax.all_to_all(curve_store, "path", split_axis=3, concat_axis=1, tiled=True)[0]
    cash_all = lax.all_gather(cash_table[None], "ccy", axis=0, tiled=True)

    def advance(unused, inputs):
        date_index, slot_id, weight_row = inputs
        remain, alive_mask, weights = date_tables(date_index, nodes, CFG)
        grid_weights = weights.astype(jnp.bfloat16)
        curve_now = lax.dynamic_index_in_dim(blocks, slot_id, 0, keepdims=False)
        curve_groups = lax.all_gather(curve_now[None], "ccy", axis=0, tiled=True)
        yields = jnp.einsum(
            "gnp,nc->gpc", curve_groups, grid_weights, preferred_element_type=jnp.float32
        )
        discount_all = alive_mask * jnp.exp(-yields * remain)
        values = jnp.einsum(
            "gpc,gcs->ps", discount_all.astype(jnp.bfloat16), cash_all,
            preferred_element_type=jnp.float32,
        )
        discount = lax.dynamic_index_in_dim(discount_all, group_index, 0, keepdims=False)
        rooted = jnp.sqrt(values * values + SOFTEN)
        slopes = (weight_row / total_paths * 0.5 * (1.0 + values / rooted)).astype(jnp.bfloat16)
        share_values = lax.dynamic_slice_in_dim(values, group_index * share_size, share_size, 1)
        share_root = lax.dynamic_slice_in_dim(rooted, group_index * share_size, share_size, 1)
        exposure_part = jnp.sum(0.5 * (share_values + share_root), axis=0) / total_paths
        back_flow = lax.dot_general(
            slopes, cash_table, (((1,), (1,)), ((), ())), preferred_element_type=jnp.float32
        )
        node_pull = jnp.sum(back_flow * -remain * discount, axis=0)
        sens_part = jnp.dot(weights, node_pull, precision=lax.Precision.HIGHEST)
        exposure_part, sens_part = lax.psum((exposure_part, sens_part), "path")
        return (unused, (exposure_part, sens_part))

    inputs = (jnp.arange(date_slot.shape[0], dtype=jnp.int32), date_slot, default_weight)
    _, (exposure_rows, sens_rows) = lax.scan(advance, jnp.zeros((), jnp.float32), inputs)
    return (exposure_rows, sens_rows[None])


def local(curve_store, cash_index, cash_amount, trade_set, date_slot, default_weight):
    stored = curve_store.shape[1] * lax.axis_size("path")
    plan = by_slot if stored == date_slot.shape[0] else by_path
    return plan(curve_store, cash_index, cash_amount, trade_set, date_slot, default_weight)


def solution(mesh):
    in_specs = (
        P("ccy", "path", None, None),
        P("ccy", None, None),
        P("ccy", None, None),
        P("ccy", None),
        P(),
        P(),
    )
    out_specs = (P(None, "ccy"), P("ccy", None, None))
    return jax.shard_map(local, mesh=mesh, in_specs=in_specs, out_specs=out_specs, check_vma=False)
```

```python
import functools

import jax
import jax.numpy as jnp
from jax import lax
from jax.experimental import pallas as pl
from jax.experimental.pallas import tpu as pltpu
from jax.sharding import PartitionSpec as P

NSETS = 512
CFG = 1024
SOFTEN = 0.04
HORIZON = 32.0
LOG2E = 1.4426950408889634
COLS = 256


def date_tables(date_index, node_count, grid_count):
    start_time = 0.5 * (jnp.asarray(date_index).astype(jnp.float32) + 1.0)
    grid_times = HORIZON * (jnp.arange(grid_count, dtype=jnp.float32) + 1.0) / grid_count
    tenors = HORIZON * (jnp.arange(node_count, dtype=jnp.float32) + 1.0) / node_count
    remain = grid_times - start_time
    alive_mask = (remain > 0.0).astype(jnp.float32)
    clipped = jnp.clip(remain, HORIZON / node_count, HORIZON)
    weights = jnp.maximum(
        0.0, 1.0 - jnp.abs(clipped[None, :] - tenors[:, None]) * (node_count / HORIZON)
    )
    return (remain, alive_mask, weights)


def cash_kernel(rows, base_ref, index_ref, amount_ref, set_ref, out_ref, a_hi, a_lo):
    flows, trades = index_ref.shape
    nsets = out_ref.shape[1]
    wanted = lax.broadcasted_iota(jnp.int32, (rows, 128), 0) + base_ref[0]

    @pl.loop(0, trades // 128)
    def _(tile):
        cols = pl.ds(pl.multiple_of(tile * 128, 128), 128)
        total = jnp.zeros((rows, 128), jnp.float32)
        index = index_ref[:, cols]
        amount = amount_ref[:, cols]
        for k in range(flows):
            hit = wanted == index[k : k + 1, :]
            total = total + jnp.where(hit, amount[k : k + 1, :], 0.0)
        high = total.astype(jnp.bfloat16)
        a_hi[:, cols] = high
        a_lo[:, cols] = (total - high.astype(jnp.float32)).astype(jnp.bfloat16)

    sets = lax.broadcasted_iota(jnp.int32, (nsets, trades), 0)
    onehot = jnp.where(sets == set_ref[...], 1.0, 0.0).astype(jnp.bfloat16)
    dims = (((1,), (1,)), ((), ()))
    table = lax.dot_general(a_hi[...], onehot, dims, preferred_element_type=jnp.float32)
    table = table + lax.dot_general(a_lo[...], onehot, dims, preferred_element_type=jnp.float32)
    out_ref[...] = table.astype(jnp.bfloat16)


def build_cash(base, flow_index, amount, trade_sets, rows, nsets):
    flows, trades = flow_index.shape[1], flow_index.shape[0]
    vmem = pl.BlockSpec(memory_space=pltpu.VMEM)
    return pl.pallas_call(
        functools.partial(cash_kernel, rows),
        out_shape=jax.ShapeDtypeStruct((rows, nsets), jnp.bfloat16),
        in_specs=[pl.BlockSpec(memory_space=pltpu.SMEM), vmem, vmem, vmem],
        out_specs=vmem,
        scratch_shapes=[pltpu.VMEM((rows, trades), jnp.bfloat16)] * 2,
        cost_estimate=pl.CostEstimate(
            flops=4 * rows * trades * nsets, bytes_accessed=4 * trades * flows, transcendentals=0
        ),
        name="cash_rows",
    )(base, flow_index.T, amount.T, trade_sets[None, :])


def main_kernel(groups, cfg, total_paths, date_ref, curve_ref, cash_ref, dw_ref, exp_ref, sens_ref, disc):
    nodes, paths = curve_ref.shape[2], curve_ref.shape[3]
    date = date_ref[pl.program_id(0)]
    start_time = 0.5 * (date.astype(jnp.float32) + 1.0)
    step = HORIZON / cfg
    tenors = (lax.broadcasted_iota(jnp.int32, (nodes, COLS), 0).astype(jnp.float32) + 1.0) * (HORIZON / nodes)
    per_group = cfg // COLS

    def tables(block):
        at = lax.broadcasted_iota(jnp.int32, (1, COLS), 1) + block * COLS
        remain = (at.astype(jnp.float32) + 1.0) * step - start_time
        clipped = jnp.clip(remain, HORIZON / nodes, HORIZON)
        weights = jnp.maximum(0.0, 1.0 - jnp.abs(clipped - tenors) * (nodes / HORIZON))
        return remain, weights

    for block in range(per_group):
        remain, weights = tables(block)
        weights = weights.astype(jnp.bfloat16)
        scaled = remain * (-LOG2E)
        alive = remain > 0.0
        for g in range(groups):
            rate = lax.dot_general(
                curve_ref[g, 0], weights, (((0,), (0,)), ((), ())), preferred_element_type=jnp.float32
            )
            value = jnp.where(alive, jnp.exp2(rate * scaled), 0.0)
            disc[:, pl.ds(g * cfg + block * COLS, COLS)] = value.astype(jnp.bfloat16)

    values = jnp.dot(disc[...], cash_ref[...], preferred_element_type=jnp.float32)
    square = values * values + SOFTEN
    inverse = lax.rsqrt(square)
    exp_ref[0] = jnp.sum(0.5 * (values + square * inverse), axis=0, keepdims=True) / total_paths
    row = dw_ref[pl.ds(date, 1), :] / total_paths * 0.5
    slopes = (row * (1.0 + values * inverse)).astype(jnp.bfloat16)

    for g in range(groups):
        sens = jnp.zeros((8, nodes), jnp.float32)
        for block in range(per_group):
            at = g * cfg + block * COLS
            back = lax.dot_general(
                slopes, cash_ref[pl.ds(at, COLS), :], (((1,), (1,)), ((), ())),
                preferred_element_type=jnp.float32,
            )
            summed = jnp.sum(back * disc[:, pl.ds(at, COLS)].astype(jnp.float32), axis=0, keepdims=True)
            remain, weights = tables(block)
            pull = jnp.broadcast_to(summed * -remain, (8, COLS))
            weights = weights.astype(jnp.bfloat16)
            for _ in range(3):
                piece = pull.astype(jnp.bfloat16)
                pull = pull - piece.astype(jnp.float32)
                sens = sens + lax.dot_general(
                    piece, weights, (((1,), (1,)), ((), ())), preferred_element_type=jnp.float32
                )
        sens_ref[0, g : g + 1, :] = sens[0:1, :]


def run_main(dates, curves, cash, default_weight, total_paths):
    groups, slots, nodes, paths = curves.shape
    rows, nsets = cash.shape
    cfg = rows // groups
    work = slots * paths * rows * (4 * nsets + 2 * nodes)
    return pl.pallas_call(
        functools.partial(main_kernel, groups, cfg, total_paths),
        grid=(slots,),
        out_shape=[
            jax.ShapeDtypeStruct((slots, 1, nsets), jnp.float32),
            jax.ShapeDtypeStruct((slots, groups, nodes), jnp.float32),
        ],
        in_specs=[
            pl.BlockSpec(memory_space=pltpu.SMEM),
            pl.BlockSpec((groups, 1, nodes, paths), lambda s: (0, s, 0, 0)),
            pl.BlockSpec(memory_space=pltpu.VMEM),
            pl.BlockSpec(memory_space=pltpu.VMEM),
        ],
        out_specs=[
            pl.BlockSpec((1, 1, nsets), lambda s: (s, 0, 0)),
            pl.BlockSpec((1, groups, nodes), lambda s: (s, 0, 0)),
        ],
        scratch_shapes=[pltpu.VMEM((paths, rows), jnp.bfloat16)],
        cost_estimate=pl.CostEstimate(
            flops=work, bytes_accessed=rows * nsets * 2, transcendentals=slots * paths * rows
        ),
        name="price_dates",
    )(dates, curves, cash, default_weight)


def exchange_kernel(chunk_ref, curve_ref, cash_ref, curves_ref, send, recv, own):
    groups, members = cash_ref.shape[0], cash_ref.shape[1]
    share = curves_ref.shape[3]
    c, p = lax.axis_index("ccy"), lax.axis_index("path")
    levels = members // 2
    z, y = p // 2, p % 2
    sibling = c + 1 - 2 * (c % 2)
    across = (c + 2) % groups
    beside = p + 1 - 2 * y
    peers = [((c + d) % groups, p) for d in range(1, groups)] + [(c, beside)]
    peers += [(c, ((z + k) % levels) * 2 + y) for k in range(1, levels)]
    barrier = pltpu.get_barrier_semaphore()
    for peer in peers:
        pl.semaphore_signal(barrier, inc=1, device_id=peer, device_id_type=pl.DeviceIdType.MESH)
    pl.semaphore_wait(barrier, len(peers))

    started = []

    def remote(src, dst, device):
        k = len(started)
        copy = pltpu.make_async_remote_copy(
            src_ref=src, dst_ref=dst, send_sem=send.at[k], recv_sem=recv.at[k],
            device_id=device, device_id_type=pl.DeviceIdType.MESH,
        )
        copy.start()
        started.append(copy)
        return copy

    near, far, core = (c, beside), (across, p), (sibling, p)
    mine = cash_ref.at[c, p]
    up = []
    for k in range(1, levels):
        up.append((k, remote(chunk_ref, mine, (c, ((z + k) % levels) * 2 + y))))
    late = []
    for d in range(1, groups):
        t = (c + d) % groups
        cols = pl.ds(pl.multiple_of(t * share, 128), share)
        late.append(remote(curve_ref.at[:, :, cols], curves_ref.at[c], (t, p)))
    keep = [
        pltpu.make_async_copy(chunk_ref, mine, own.at[0]),
        pltpu.make_async_copy(
            curve_ref.at[:, :, pl.ds(pl.multiple_of(c * share, 128), share)], curves_ref.at[c], own.at[1]
        ),
    ]
    for copy in keep:
        copy.start()

    second = []

    def spread(source, q):
        other = q + 1 - 2 * y
        a = remote(source.at[0], cash_ref.at[c, q, 0], near)
        b = remote(source.at[1], cash_ref.at[c, q, 1], far)
        second.append((a, b, q, other))
        late.append(remote(source.at[0], cash_ref.at[c, q, 0], far))
        late.append(remote(source.at[1], cash_ref.at[c, q, 1], near))
        late.append(remote(source, cash_ref.at[c, q], core))

    third = []
    spread(chunk_ref, p)
    for k, copy in up:
        copy.wait_recv()
        q = ((z - k + levels) % levels) * 2 + y
        spread(cash_ref.at[c, q], q)
    for a, b, q, other in second:
        a.wait_recv()
        block = cash_ref.at[c, other, 0]
        third.append((remote(block, block, far), cash_ref.at[across, other, 0]))
        late.append(remote(block, block, core))
        b.wait_recv()
        block = cash_ref.at[across, q, 1]
        third.append((remote(block, block, near), cash_ref.at[across, other, 1]))
        late.append(remote(block, block, core))
    first = 0
    for a, b, q, other in second:
        base = len(up) + groups - 1 + 5 * first
        first += 1
        started[base + 2].wait_recv()
        block = cash_ref.at[across, q, 0]
        late.append(remote(block, block, core))
        started[base + 3].wait_recv()
        block = cash_ref.at[c, other, 1]
        late.append(remote(block, block, core))
    for copy, block in third:
        copy.wait_recv()
        late.append(remote(block, block, core))
    passed = {id(started[len(up) + groups - 1 + 5 * n + m]) for n in range(levels) for m in (2, 3)}
    for copy in late:
        if id(copy) not in passed:
            copy.wait_recv()
    for copy in started:
        copy.wait_send()
    for copy in keep:
        copy.wait()


def exchange(chunk, curve_store, groups, members):
    rows, nsets = chunk.shape
    _, slots, nodes, paths = curve_store.shape
    levels = members // 2
    count = levels - 1 + groups - 1 + 5 * levels + 4 * levels + 2 * levels + 2 * levels
    hbm = pl.BlockSpec(memory_space=pl.ANY)
    vmem = pl.BlockSpec(memory_space=pltpu.VMEM)
    cash, curves = pl.pallas_call(
        exchange_kernel,
        out_shape=[
            jax.ShapeDtypeStruct((groups, members, 2, rows // 2, nsets), chunk.dtype),
            jax.ShapeDtypeStruct((groups, slots, nodes, paths // groups), curve_store.dtype),
        ],
        in_specs=[vmem, vmem],
        out_specs=[hbm, hbm],
        scratch_shapes=[
            pltpu.SemaphoreType.DMA((count,)),
            pltpu.SemaphoreType.DMA((count,)),
            pltpu.SemaphoreType.DMA((2,)),
        ],
        compiler_params=pltpu.CompilerParams(collective_id=0, has_side_effects=True),
        name="exchange",
    )(chunk.reshape(2, rows // 2, nsets), curve_store[0])
    return cash.reshape(groups * members * rows, nsets), curves


def collect_kernel(groups, members, part_ref, out_ref, held, send, recv, own):
    c, p = lax.axis_index("ccy"), lax.axis_index("path")
    steps = [(dc, dp) for dc in range(groups) for dp in range(members)][1:]
    barrier = pltpu.get_barrier_semaphore()
    targets = [((c + dc) % groups, (p + dp) % members) for dc, dp in steps]
    for target in targets:
        pl.semaphore_signal(barrier, inc=1, device_id=target, device_id_type=pl.DeviceIdType.MESH)
    keep = pltpu.make_async_copy(part_ref.at[c], held.at[c, p], own.at[0])
    keep.start()
    pl.semaphore_wait(barrier, len(targets))
    copies = []
    for k, target in enumerate(targets):
        copy = pltpu.make_async_remote_copy(
            src_ref=part_ref.at[target[0]], dst_ref=held.at[c, p], send_sem=send.at[k],
            recv_sem=recv.at[k], device_id=target, device_id_type=pl.DeviceIdType.MESH,
        )
        copy.start()
        copies.append(copy)
    keep.wait()
    for copy in copies:
        copy.wait()
    total = held[0]
    for g in range(1, groups):
        total = total + held[g]
    out_ref[...] = total


def collect(part, members):
    groups = part.shape[0]
    links = groups * members - 1
    vmem = pl.BlockSpec(memory_space=pltpu.VMEM)
    return pl.pallas_call(
        functools.partial(collect_kernel, groups, members),
        out_shape=jax.ShapeDtypeStruct((members,) + part.shape[1:], jnp.float32),
        in_specs=[vmem],
        out_specs=vmem,
        scratch_shapes=[
            pltpu.VMEM((groups, members) + part.shape[1:], jnp.float32),
            pltpu.SemaphoreType.DMA((links,)),
            pltpu.SemaphoreType.DMA((links,)),
            pltpu.SemaphoreType.DMA((1,)),
        ],
        compiler_params=pltpu.CompilerParams(collective_id=1, has_side_effects=True),
        name="collect",
    )(part)


def by_slot(curve_store, cash_index, cash_amount, trade_set, date_slot, default_weight):
    groups, members = lax.axis_size("ccy"), lax.axis_size("path")
    path_index = lax.axis_index("path")
    slots = curve_store.shape[1]
    nodes = curve_store.shape[2]
    total_paths = curve_store.shape[3]
    rows = CFG // members
    nsets = default_weight.shape[1]
    base = (path_index * rows).astype(jnp.int32)[None]
    chunk = build_cash(base, cash_index[0], cash_amount[0], trade_set[0], rows, nsets)
    if groups == 4 and members % 2 == 0:
        cash, curves = exchange(chunk, curve_store, groups, members)
    else:
        curves = lax.all_to_all(curve_store, "ccy", split_axis=3, concat_axis=0, tiled=True)
        cash = lax.all_gather(chunk, ("ccy", "path"), axis=0, tiled=True)
    own = path_index * slots + jnp.arange(slots, dtype=jnp.int32)
    numbers = jnp.arange(date_slot.shape[0], dtype=jnp.int32)
    dates = jnp.sum(jnp.where(date_slot[None, :] == own[:, None], numbers[None, :], 0), axis=1).astype(jnp.int32)
    exposure_part, sens_part = run_main(dates, curves, cash, default_weight, total_paths)
    share = nsets // groups
    exposure_part = jnp.transpose(exposure_part.reshape(slots, groups, share), (1, 0, 2))
    sens_part = jnp.transpose(sens_part, (1, 0, 2))
    sens_part = jnp.pad(sens_part, ((0, 0), (0, 0), (0, max(share - nodes, 0))))
    exposure_part = jnp.pad(exposure_part, ((0, 0), (0, 0), (0, max(nodes - share, 0))))
    part = jnp.concatenate([exposure_part, sens_part], axis=1)
    part = jnp.pad(part, ((0, 0), (0, -2 * slots % 8), (0, 0)))
    sums = collect(part, members)
    hit = date_slot[:, None, None] == jnp.arange(members * slots, dtype=jnp.int32)[None, :, None]

    def finish(block):
        return jnp.sum(jnp.where(hit, block.reshape(1, members * slots, -1), 0.0), axis=1)

    exposure = finish(sums[:, :slots, :share])
    sens = finish(sums[:, slots : 2 * slots, :nodes])
    return (exposure, sens[None])


def by_path(curve_store, cash_index, cash_amount, trade_set, date_slot, default_weight):
    groups = lax.axis_size("ccy")
    group_index = lax.axis_index("ccy")
    members = lax.axis_size("path")
    nodes, total_paths = curve_store.shape[2], curve_store.shape[3]
    nsets = default_weight.shape[1]
    share_size = nsets // groups
    rows = CFG // members
    base = (lax.axis_index("path") * rows).astype(jnp.int32)[None]
    chunk = build_cash(base, cash_index[0], cash_amount[0], trade_set[0], rows, nsets)
    cash_table = lax.all_gather(chunk, "path", axis=0, tiled=True)
    blocks = lax.all_to_all(curve_store, "path", split_axis=3, concat_axis=1, tiled=True)[0]
    cash_all = lax.all_gather(cash_table[None], "ccy", axis=0, tiled=True)

    def advance(unused, inputs):
        date_index, slot_id, weight_row = inputs
        remain, alive_mask, weights = date_tables(date_index, nodes, CFG)
        grid_weights = weights.astype(jnp.bfloat16)
        curve_now = lax.dynamic_index_in_dim(blocks, slot_id, 0, keepdims=False)
        curve_groups = lax.all_gather(curve_now[None], "ccy", axis=0, tiled=True)
        yields = jnp.einsum(
            "gnp,nc->gpc", curve_groups, grid_weights, preferred_element_type=jnp.float32
        )
        discount_all = alive_mask * jnp.exp(-yields * remain)
        values = jnp.einsum(
            "gpc,gcs->ps", discount_all.astype(jnp.bfloat16), cash_all,
            preferred_element_type=jnp.float32,
        )
        discount = lax.dynamic_index_in_dim(discount_all, group_index, 0, keepdims=False)
        rooted = jnp.sqrt(values * values + SOFTEN)
        slopes = (weight_row / total_paths * 0.5 * (1.0 + values / rooted)).astype(jnp.bfloat16)
        share_values = lax.dynamic_slice_in_dim(values, group_index * share_size, share_size, 1)
        share_root = lax.dynamic_slice_in_dim(rooted, group_index * share_size, share_size, 1)
        exposure_part = jnp.sum(0.5 * (share_values + share_root), axis=0) / total_paths
        back_flow = lax.dot_general(
            slopes, cash_table, (((1,), (1,)), ((), ())), preferred_element_type=jnp.float32
        )
        node_pull = jnp.sum(back_flow * -remain * discount, axis=0)
        sens_part = jnp.dot(weights, node_pull, precision=lax.Precision.HIGHEST)
        exposure_part, sens_part = lax.psum((exposure_part, sens_part), "path")
        return (unused, (exposure_part, sens_part))

    inputs = (jnp.arange(date_slot.shape[0], dtype=jnp.int32), date_slot, default_weight)
    _, (exposure_rows, sens_rows) = lax.scan(advance, jnp.zeros((), jnp.float32), inputs)
    return (exposure_rows, sens_rows[None])


def local(curve_store, cash_index, cash_amount, trade_set, date_slot, default_weight):
    stored = curve_store.shape[1] * lax.axis_size("path")
    plan = by_slot if stored == date_slot.shape[0] else by_path
    return plan(curve_store, cash_index, cash_amount, trade_set, date_slot, default_weight)


def solution(mesh):
    in_specs = (
        P("ccy", "path", None, None),
        P("ccy", None, None),
        P("ccy", None, None),
        P("ccy", None),
        P(),
        P(),
    )
    out_specs = (P(None, "ccy"), P("ccy", None, None))
    return jax.shard_map(local, mesh=mesh, in_specs=in_specs, out_specs=out_specs, check_vma=False)
```
